32 devices in a mesh: seq: 8 (over y, x, core), tp: 4 (over z).
Axes of the slice: x: 2, y: 2, z: 4, core: 2. Of those that a mesh axis runs over, the one named last changes fastest.
Arguments:
- inputs: bfloat16 [2048, 5120], P('seq', 'tp'), may hold values from -6 to 6
- gate_input: bfloat16 [2048, 5120], P('seq', 'tp'), may hold values from -6 to 6
- b_source: bfloat16 [2048, 128], P('seq'), may hold values from -6 to 6
- c_source: bfloat16 [2048, 128], P('seq'), may hold values from -6 to 6
- step_raw: float32 [2048, 80], P('seq', 'tp'), may hold values from -4 to 4
- step_bias: float32 [80], P('tp'), may hold values from -3 to 0
- decay_rate: float32 [80], P('tp'), may hold values from 9.765625e-05 to 0.05
- conv_weight: float32 [4, 256], replicated, may hold values from -3 to 3
- conv_bias: float32 [256], replicated, may hold values from -3 to 3
- norm_gain: float32 [5120], P('tp'), may hold values from 0.5 to 1.5
- doc_lengths: int32 [8], replicated, may hold values from 1 to 1024, 2048 in all
Outputs:
- output: bfloat16 [2048, 5120], P('seq', 'tp')
The draws below stay inside these ranges and needn't reach their ends.
Inputs may be any that keep to these rules, and one draw needn't show every extreme that they name: doc_lengths sums to 2048; every length is at least 1 and the largest is exactly 1024.
All inputs are finite; a program needn't handle non-finite values.
Results may differ from the reference program's by a relative error of at most 0.0015.
Values may be sent and summed in bfloat16 or wider, within the bound.
A program may use at most 192 MiB of HBM per device.

```python
import math
import jax
import jax.numpy as jnp
import numpy as np
from jax import lax

H = 80
HEAD_DIM = 64
STATE = 128
CONV = 4
BLOCK = 256
DOCS = 8
SEQ = 2048
DOC_MOST = 1024


def steps_of(key, dims, shards, low, top_value):
    factor_of = 1.0
    for dim, shards_of in shards:
        steps = jax.random.uniform(jax.random.fold_in(jax.random.fold_in(key, 6), dim), (shards_of,), jnp.float32, low / len(shards), top_value / len(shards))
        factor_of = factor_of * jnp.repeat(jnp.exp(steps), dims[dim] // shards_of).reshape((-1,) + (1,) * (len(dims) - 1 - dim))
    return factor_of


def profile(number_of, total, bound, skew):
    loads = [(1 << 20) // math.isqrt(grade ** skew) + 1 for grade in range(2, number_of + 1)]
    surplus, holding = total - bound - (number_of - 1), [1] * (number_of - 1)
    while surplus > 0:
        candidates = [i for i in range(number_of - 1) if holding[i] < bound]
        pool, left = sum([loads[i] for i in candidates]), surplus
        for i in candidates:
            more = min(bound - holding[i], max(1, left * loads[i] // pool), surplus)
            holding[i] = holding[i] + more
            surplus = surplus - more
    return np.array([bound] + holding)


def ragged_sizes(rng, number_of, total, most, slope):
    if number_of == 2:
        one = jax.random.randint(rng, (), max(1, total - most), min(most, total - 1) + 1)
        return jnp.stack([one, total - one])
    lengths = jnp.asarray(profile(number_of, total, most, slope), jnp.int32)
    couples = (number_of - 1) // 2
    giver, sink = lengths[1:1 + 2 * couples:2], lengths[2:2 + 2 * couples:2]
    slack = jnp.minimum(giver - 1, most - sink)
    passed = jax.random.randint(jax.random.fold_in(rng, 1), (couples,), 0, 1 << 20) % (slack + 1)
    lengths = lengths.at[1:1 + 2 * couples:2].set(giver - passed).at[2:2 + 2 * couples:2].set(sink + passed)
    return lengths[jax.random.permutation(jax.random.fold_in(rng, 2), number_of)]


def normal_values(stream_key, extent, spread, reach, cuts=(), held_as=jnp.bfloat16):
    drawn = spread * jax.random.normal(stream_key, extent, jnp.float32)
    if cuts:
        drawn = drawn * steps_of(stream_key, extent, cuts, -0.22, 0.18)
    return jnp.clip(drawn, -reach, reach).astype(held_as)


def setup_inputs(seed: int = 0) -> dict:
    key_of = jax.random.split(jax.random.key(seed), 12)
    inputs = normal_values(key_of[0], (SEQ, H * HEAD_DIM), 1.0, 6.0, ((0, 8), (1, 4)))
    gate_input = normal_values(key_of[1], (SEQ, H * HEAD_DIM), 1.0, 6.0, ((0, 8), (1, 4)))
    b_source = normal_values(key_of[2], (SEQ, STATE), 1.0, 6.0, ((0, 8),))
    c_source = normal_values(key_of[3], (SEQ, STATE), 1.0, 6.0, ((0, 8),))
    step_raw = normal_values(key_of[4], (SEQ, H), 0.5, 4.0, ((0, 8), (1, 4)), jnp.float32)
    step_bias = jnp.clip(-3.0 + 3.0 * jax.random.uniform(key_of[5], (H,), jnp.float32) ** steps_of(key_of[5], (H,), ((0, 4),), -0.2, 0.2), -3.0, 0.0)
    decay_rate = jnp.clip(jnp.exp(math.log(0.05) - 6.2383246 * jax.random.uniform(key_of[6], (H,), jnp.float32) ** steps_of(key_of[6], (H,), ((0, 4),), -0.2, 0.2)), 9.765625145519152e-05, 0.05)
    conv_weight = normal_values(key_of[7], (CONV, 2 * STATE), CONV ** -0.5, 3.0, (), jnp.float32)
    conv_bias = normal_values(key_of[8], (2 * STATE,), 0.5, 3.0, (), jnp.float32)
    norm_gain = jnp.clip(1.0 + 0.1 * jax.random.normal(key_of[9], (H * HEAD_DIM,), jnp.float32), 0.5, 1.5)
    doc_lengths = ragged_sizes(key_of[10], DOCS, SEQ, DOC_MOST, 2).astype(jnp.int32)
    return {"inputs": inputs, "gate_input": gate_input, "b_source": b_source, "c_source": c_source, "step_raw": step_raw, "step_bias": step_bias, "decay_rate": decay_rate, "conv_weight": conv_weight, "conv_bias": conv_bias, "norm_gain": norm_gain, "doc_lengths": doc_lengths}


epsilon = 1e-05

def locate(position, doc_lengths):
    starts = (jnp.cumsum(doc_lengths) - doc_lengths).astype(jnp.int32)
    chosen = jnp.where(starts[None, :] <= position[:, None], starts[None, :], 0)
    return lax.optimization_barrier(jnp.max(chosen, axis=1)).astype(jnp.int32)

def convolve(padded, weight, conv_bias, position, doc_start):
    kernel_taps = weight.shape[0]
    tokens = position.shape[0]
    widened = padded.astype(jnp.float32)
    summed = jnp.broadcast_to(conv_bias[None, :], (tokens, conv_bias.shape[0]))
    for offset in range(kernel_taps):
        backward = kernel_taps - 1 - offset
        inside = (position - backward >= doc_start)[:, None]
        summed = summed + jnp.where(inside, weight[offset][None, :] * widened[offset:offset + tokens], 0.0)
    return jax.nn.silu(summed).astype(jnp.bfloat16)

def state_terms(pieces):
    block_inputs, b_block, step_size, cumulated, doc_start, position = pieces
    same_doc = doc_start == doc_start[-1]
    weighting = jnp.where(same_doc[:, None], jnp.exp(cumulated[-1][None, :] - cumulated) * step_size, 0.0)
    weighted = (block_inputs.astype(jnp.float32) * weighting[:, :, None]).astype(jnp.bfloat16)
    weighted = lax.optimization_barrier(weighted).astype(jnp.float32)
    end_state = jnp.einsum('qhp,qn->hpn', weighted, b_block.astype(jnp.float32), precision=lax.Precision.HIGHEST)
    end_factor = jnp.where(doc_start[-1] < position[0], jnp.exp(cumulated[-1]), 0.0)
    return (end_state, end_factor)

def diagonal_terms(pieces):
    block_inputs, b_block, c_block, step_size, cumulated, doc_start = pieces
    row_count = doc_start.shape[0]
    products = jnp.dot(c_block, b_block.T, preferred_element_type=jnp.float32)
    order_ids = jnp.arange(row_count)
    causal = (order_ids[None, :] <= order_ids[:, None]) & (doc_start[None, :] == doc_start[:, None])
    decay_gap = cumulated.T[:, :, None] - cumulated.T[:, None, :]
    scores = jnp.where(causal[None], products[None] * jnp.exp(decay_gap) * step_size.T[:, None, :], 0.0)
    scores = lax.optimization_barrier(scores.astype(jnp.bfloat16)).astype(jnp.float32)
    return jnp.einsum('hts,shp->thp', scores, block_inputs.astype(jnp.float32), precision=lax.Precision.HIGHEST)

def emit_rows(state_in, pieces):
    end_state, end_factor, c_block, out_decay = pieces
    rounded = lax.optimization_barrier(state_in.astype(jnp.bfloat16)).astype(jnp.float32)
    from_state = jnp.einsum('qn,hpn->qhp', c_block.astype(jnp.float32), rounded, precision=lax.Precision.HIGHEST)
    from_state = from_state * out_decay[:, :, None]
    return (end_factor[:, None, None] * state_in + end_state, from_state)

def reference(inputs, gate_input, b_source, c_source, step_raw, step_bias, decay_rate, conv_weight, conv_bias, norm_gain, doc_lengths):
    position = jnp.arange(SEQ, dtype=jnp.int32)
    doc_start = locate(position, doc_lengths)
    keep_rows = CONV - 1
    blank = jnp.zeros((keep_rows, STATE), jnp.bfloat16)
    b_conv = convolve(jnp.concatenate([blank, b_source], 0), conv_weight[:, :STATE], conv_bias[:STATE], position, doc_start)
    c_conv = convolve(jnp.concatenate([blank, c_source], 0), conv_weight[:, STATE:], conv_bias[STATE:], position, doc_start)
    step_size = jax.nn.softplus(step_raw + step_bias[None, :])
    log_decay = -step_size * decay_rate[None, :]
    block_count = SEQ // BLOCK
    shaped_inputs = inputs.reshape(block_count, BLOCK, H, HEAD_DIM)
    b_blocks = b_conv.reshape(block_count, BLOCK, STATE)
    c_blocks = c_conv.reshape(block_count, BLOCK, STATE)
    step_blocks = step_size.reshape(block_count, BLOCK, H)
    cumulated = jnp.cumsum(log_decay.reshape(block_count, BLOCK, H), axis=1)
    start_blocks = doc_start.reshape(block_count, BLOCK)
    position_blocks = position.reshape(block_count, BLOCK)
    out_decay = jnp.where((start_blocks < position_blocks[:, :1])[:, :, None], jnp.exp(cumulated), 0.0)

    def advance(state_in, pieces):
        block_inputs, b_block, c_block, step_block, cum_block, start_block, position_block, decay_block = pieces
        end_state, end_factor = state_terms((block_inputs, b_block, step_block, cum_block, start_block, position_block))
        diagonal = diagonal_terms((block_inputs, b_block, c_block, step_block, cum_block, start_block))
        next_state, from_state = emit_rows(state_in, (end_state, end_factor, c_block, decay_block))
        return (next_state, diagonal + from_state)
    initial = jnp.zeros((H, HEAD_DIM, STATE), jnp.float32)
    final_state, mixed = lax.scan(advance, initial, (shaped_inputs, b_blocks, c_blocks, step_blocks, cumulated, start_blocks, position_blocks, out_decay))
    mixed = mixed.reshape(SEQ, H * HEAD_DIM)
    gated = mixed * jax.nn.silu(gate_input.astype(jnp.float32))
    mean_square = lax.optimization_barrier(jnp.sum(gated * gated, axis=1)) / (H * HEAD_DIM)
    return (gated * lax.rsqrt(mean_square + epsilon)[:, None] * norm_gain[None, :]).astype(jnp.bfloat16)
```

```python
import functools

import jax
import jax.numpy as jnp
from jax import lax
from jax.experimental import pallas as pl
from jax.experimental.pallas import tpu as pltpu
from jax.sharding import PartitionSpec as P

MESH = pl.DeviceIdType.MESH
LANES = 128
TILE = 8
ROWS16 = 16
epsilon = 1e-05


def kernel(
    seq_n,
    tp_n,
    head_width,
    inputs,
    gate_input,
    b_source,
    c_source,
    step_raw,
    step_bias,
    decay_rate,
    conv_weight,
    conv_bias,
    norm_gain,
    doc_lengths,
    output,
    xs,
    gates,
    source,
    halo,
    padded,
    own,
    from_pair,
    totals,
    received,
    prefixes,
    leaving,
    arrived,
    masked,
    mixed,
    gate_decay,
    squares,
    local_sem,
    halo_send,
    halo_recv,
    state_send,
    state_recv,
    square_send,
    square_recv,
):
    tokens = inputs.shape[0]
    chunks = xs.shape[0]
    half = chunks // 2
    state_width = b_source.shape[1]
    taps = conv_weight.shape[0]
    bits = seq_n.bit_length() - 1
    me = lax.axis_index("seq")
    mine = lax.axis_index("tp")
    odd = lax.rem(me, 2)
    rows = state_width

    copies = [
        pltpu.make_async_copy(b_source, source.at[0], local_sem.at[0]),
        pltpu.make_async_copy(c_source, source.at[1], local_sem.at[1]),
    ]
    for copy in copies:
        copy.start()
    x_copies, gate_copies = [], []
    for j in range(chunks):
        lanes = pl.ds(j * LANES, LANES)
        x_copies.append(
            pltpu.make_async_copy(inputs.at[:, lanes], xs.at[j], local_sem.at[2 + j])
        )
        x_copies[-1].start()
    for j in range(chunks):
        lanes = pl.ds(j * LANES, LANES)
        gate_copies.append(
            pltpu.make_async_copy(
                gate_input.at[:, lanes], gates.at[j], local_sem.at[2 + chunks + j]
            )
        )
        gate_copies[-1].start()

    after = lax.rem(me + 1, seq_n)
    before = lax.rem(me + seq_n - 1, seq_n)
    partners = []
    for bit in range(bits):
        stride = 1 << bit
        partners.append(me + (1 - 2 * lax.rem(me // stride, 2)) * stride)
    barrier = pltpu.get_barrier_semaphore()
    for device in [after, before] + partners:
        pl.semaphore_signal(barrier, inc=1, device_id={"seq": device}, device_id_type=MESH)
    for ahead in range(1, tp_n):
        pl.semaphore_signal(
            barrier,
            inc=1,
            device_id={"tp": lax.rem(mine + ahead, tp_n)},
            device_id_type=MESH,
        )
    pl.semaphore_wait(barrier, 2 + bits + tp_n - 1)

    for copy in copies:
        copy.wait()
    halos = []
    for k in range(2):
        halos.append(
            pltpu.make_async_remote_copy(
                src_ref=source.at[k, pl.ds(tokens - ROWS16, ROWS16)],
                dst_ref=halo.at[k],
                send_sem=halo_send.at[k],
                recv_sem=halo_recv.at[k],
                device_id={"seq": after},
                device_id_type=MESH,
            )
        )
        halos[-1].start()

    first = me * tokens
    starts = []
    running = jnp.int32(0)
    for i in range(doc_lengths.shape[0]):
        starts.append(running)
        running = running + doc_lengths[i]

    def locate(position):
        chosen = jnp.zeros_like(position)
        for start in starts:
            chosen = jnp.maximum(chosen, jnp.where(position >= start, start, 0))
        return chosen

    position = first + lax.broadcasted_iota(jnp.int32, (tokens, LANES), 0)
    doc_start = locate(position)
    row_start = locate(first + lax.broadcasted_iota(jnp.int32, (TILE, tokens), 1))[:1]
    end_start = doc_start[tokens - 1 :, :1]

    step_size = jax.nn.softplus(step_raw[...] + step_bias[...])
    log_decay = -step_size * decay_rate[...]
    row_ids = lax.broadcasted_iota(jnp.int32, (tokens, tokens), 0)
    column_ids = lax.broadcasted_iota(jnp.int32, (tokens, tokens), 1)
    causal = column_ids <= row_ids
    cumulated = jnp.dot(
        causal.astype(jnp.float32),
        log_decay,
        precision=lax.Precision.HIGHEST,
        preferred_element_type=jnp.float32,
    )
    heads = step_raw.shape[1]
    last = cumulated[tokens - 1 :]
    weighting = jnp.where(
        doc_start[:, :heads] == end_start, jnp.exp(last - cumulated) * step_size, 0.0
    )
    grow = jnp.exp(cumulated)
    out_decay = jnp.where(doc_start[:, :heads] < first, grow, 0.0)
    factor = jnp.where(end_start < first, jnp.exp(last), 0.0)
    shrink = jnp.transpose(jnp.exp(-cumulated) * step_size)
    low_half = lax.broadcasted_iota(jnp.int32, (1, LANES), 1) < head_width
    low_mask = low_half.astype(jnp.float32).astype(jnp.bfloat16)
    high_mask = (1.0 - low_half.astype(jnp.float32)).astype(jnp.bfloat16)

    def spread(values, j):
        return jnp.where(low_half, values[:, 2 * j : 2 * j + 1], values[:, 2 * j + 1 : 2 * j + 2])

    for copy in halos:
        copy.wait()
    convolved = []
    for k in range(2):
        lanes = slice(k * state_width, (k + 1) * state_width)
        padded[k, 0:ROWS16, :] = halo[k].astype(jnp.float32)
        padded[k, ROWS16 : ROWS16 + tokens, :] = source[k].astype(jnp.float32)
        summed = jnp.broadcast_to(conv_bias[:, lanes], (tokens, state_width))
        for offset in range(taps):
            backward = taps - 1 - offset
            begin = ROWS16 - backward
            term = conv_weight[offset : offset + 1, lanes] * padded[k, begin : begin + tokens, :]
            summed = summed + jnp.where(position - backward >= doc_start, term, 0.0)
        convolved.append(jax.nn.silu(summed))
    b_conv = convolved[0].astype(jnp.bfloat16)
    c_conv = convolved[1].astype(jnp.bfloat16)
    b_across = jnp.transpose(convolved[0]).astype(jnp.bfloat16)

    def send(src, dst, stage, i, partner):
        return pltpu.make_async_remote_copy(
            src_ref=src,
            dst_ref=dst,
            send_sem=state_send.at[stage, i],
            recv_sem=state_recv.at[stage, i],
            device_id={"seq": partner},
            device_id_type=MESH,
        )

    for j in range(chunks):
        x_copies[j].wait()
        weighted = (xs[j].astype(jnp.float32) * spread(weighting, j)).astype(jnp.bfloat16)
        own[j, :rows] = jnp.dot(b_across, weighted, preferred_element_type=jnp.float32)
        own[j, rows:] = jnp.broadcast_to(spread(factor, j), (TILE, LANES))
    pair = []
    for i in range(half):
        pair.append(send(own.at[(1 - odd) * half + i], from_pair.at[i], 0, i, partners[0]))
        pair[-1].start()

    products = lax.dot_general(
        c_conv, b_conv, (((1,), (1,)), ((), ())), preferred_element_type=jnp.float32
    )
    masked[...] = jnp.where(causal & (doc_start[:, :1] == row_start), products, 0.0)

    def diagonal(j):
        total = None
        x = xs[j]
        for k, mask in enumerate((low_mask, high_mask)):
            h = 2 * j + k
            scores = masked[...] * grow[:, h : h + 1] * shrink[h : h + 1, :]
            part = jnp.dot(
                scores.astype(jnp.bfloat16), x * mask, preferred_element_type=jnp.float32
            )
            total = part if total is None else total + part
        gate_copies[j].wait()
        gate = jax.nn.silu(gates[j].astype(jnp.float32))
        mixed[j] = total * gate
        gate_decay[j] = gate * spread(out_decay, j)

    def pending(stage):
        return [
            send(totals.at[stage - 1, i], received.at[stage - 1, i], stage, i, partners[stage])
            for i in range(half)
        ]

    stages = {stage: pending(stage) for stage in range(1, bits)}
    evens = []
    for i in range(half):
        pair[i].wait()
        m = own[odd * half + i]
        p = from_pair[i]
        even = jnp.where(odd == 0, m, p)
        later = jnp.where(odd == 0, p, m)
        totals[0, i, :rows] = later[rows : rows + 1] * even[:rows] + later[:rows]
        totals[0, i, rows:] = later[rows:] * even[rows:]
        stages[1][i].start()

    def finish(j, state):
        from_state = jnp.dot(c_conv, state, preferred_element_type=jnp.float32)
        gated = mixed[j] + from_state * gate_decay[j]
        mixed[j] = gated
        return gated * gated

    done = 0
    last_stage = bits - 1
    square = jnp.zeros((tokens, LANES), jnp.float32)
    final = [send(leaving.at[i], arrived.at[i], bits, i, partners[0]) for i in range(half)]
    for stage in range(1, bits):
        bit = lax.rem(me // (1 << stage), 2)
        for i in range(half):
            while done < min(chunks, 2 * (i + 1)):
                diagonal(done)
                done += 1
            stages[stage][i].wait()
            p_state, p_factor = received[stage - 1, i, :rows], received[stage - 1, i, rows:]
            if stage < last_stage:
                m_state, m_factor = totals[stage - 1, i, :rows], totals[stage - 1, i, rows:]
                totals[stage, i, :rows] = jnp.where(
                    bit == 1, m_factor[:1] * p_state + m_state, p_factor[:1] * m_state + p_state
                )
                totals[stage, i, rows:] = m_factor * p_factor
                stages[stage + 1][i].start()
            if stage == 1:
                prefix = jnp.where(bit == 1, p_state, 0.0)
                prefix_factor = jnp.where(bit == 1, p_factor, 1.0)
            else:
                prefix, prefix_factor = prefixes[i, :rows], prefixes[i, rows:]
                prefix = jnp.where(bit == 1, prefix_factor[:1] * p_state + prefix, prefix)
                prefix_factor = jnp.where(bit == 1, prefix_factor * p_factor, prefix_factor)
            if stage < last_stage:
                prefixes[i, :rows] = prefix
                prefixes[i, rows:] = prefix_factor
                continue
            mine_here = own[odd * half + i]
            theirs = from_pair[i]
            even = jnp.where(odd == 0, mine_here, theirs)
            follows = even[rows : rows + 1] * prefix + even[:rows]
            leaving[i] = jnp.where(odd == 0, follows, prefix).astype(jnp.bfloat16)
            final[i].start()
            kept = jnp.where(odd == 0, prefix, follows).astype(jnp.bfloat16)
            square = square + finish(odd * half + i, kept)
    for i in range(half):
        final[i].wait()
        square = square + finish((1 - odd) * half + i, arrived[i])

    across = jnp.sum(jnp.transpose(square), axis=0, keepdims=True)
    squares[0] = jnp.broadcast_to(across, (TILE, tokens))
    sums = []
    for ahead in range(1, tp_n):
        sums.append(
            pltpu.make_async_remote_copy(
                src_ref=squares.at[0],
                dst_ref=squares.at[ahead],
                send_sem=square_send.at[ahead - 1],
                recv_sem=square_recv.at[ahead - 1],
                device_id={"tp": lax.rem(mine + ahead, tp_n)},
                device_id_type=MESH,
            )
        )
        sums[-1].start()
    for copy in sums:
        copy.wait()
    total = squares[0]
    for ahead in range(1, tp_n):
        total = total + squares[ahead]
    mean_square = total / (chunks * LANES * tp_n)
    scale = jnp.transpose(lax.rsqrt(mean_square + epsilon))[:, :1]
    for j in range(chunks):
        lanes = slice(j * LANES, (j + 1) * LANES)
        output[:, lanes] = (mixed[j] * scale * norm_gain[:, lanes]).astype(jnp.bfloat16)


def per_device(
    inputs,
    gate_input,
    b_source,
    c_source,
    step_raw,
    step_bias,
    decay_rate,
    conv_weight,
    conv_bias,
    norm_gain,
    doc_lengths,
):
    tokens, width = inputs.shape
    head_count = step_raw.shape[1]
    head_width = width // head_count
    state_width = b_source.shape[1]
    chunks = width // LANES
    half = chunks // 2
    seq_n, tp_n = lax.axis_size("seq"), lax.axis_size("tp")
    bits = seq_n.bit_length() - 1
    message = state_width + TILE
    whole = pl.BlockSpec(memory_space=pl.ANY)
    vmem = pl.BlockSpec(memory_space=pltpu.VMEM)
    f32, bf16 = jnp.float32, jnp.bfloat16
    return pl.pallas_call(
        functools.partial(kernel, seq_n, tp_n, head_width),
        out_shape=jax.ShapeDtypeStruct((tokens, width), bf16),
        in_specs=[whole] * 4 + [vmem] * 6 + [pl.BlockSpec(memory_space=pltpu.SMEM)],
        out_specs=vmem,
        scratch_shapes=[
            pltpu.VMEM((chunks, tokens, LANES), bf16),
            pltpu.VMEM((chunks, tokens, LANES), bf16),
            pltpu.VMEM((2, tokens, state_width), bf16),
            pltpu.VMEM((2, ROWS16, state_width), bf16),
            pltpu.VMEM((2, tokens + ROWS16, state_width), f32),
            pltpu.VMEM((chunks, message, LANES), f32),
            pltpu.VMEM((half, message, LANES), f32),
            pltpu.VMEM((bits - 1, half, message, LANES), f32),
            pltpu.VMEM((bits - 1, half, message, LANES), f32),
            pltpu.VMEM((half, message, LANES), f32),
            pltpu.VMEM((half, state_width, LANES), bf16),
            pltpu.VMEM((half, state_width, LANES), bf16),
            pltpu.VMEM((tokens, tokens), f32),
            pltpu.VMEM((chunks, tokens, LANES), f32),
            pltpu.VMEM((chunks, tokens, LANES), f32),
            pltpu.VMEM((tp_n, TILE, tokens), f32),
            pltpu.SemaphoreType.DMA((2 + 2 * chunks,)),
            pltpu.SemaphoreType.DMA((2,)),
            pltpu.SemaphoreType.DMA((2,)),
            pltpu.SemaphoreType.DMA((bits + 1, half)),
            pltpu.SemaphoreType.DMA((bits + 1, half)),
            pltpu.SemaphoreType.DMA((tp_n - 1,)),
            pltpu.SemaphoreType.DMA((tp_n - 1,)),
        ],
        compiler_params=pltpu.CompilerParams(
            collective_id=0, has_side_effects=True, vmem_limit_bytes=60000 * 1024
        ),
    )(
        inputs,
        gate_input,
        b_source,
        c_source,
        step_raw,
        step_bias[None, :],
        decay_rate[None, :],
        conv_weight,
        conv_bias[None, :],
        norm_gain[None, :],
        doc_lengths,
    )


def solution(mesh):
    return jax.shard_map(
        per_device,
        mesh=mesh,
        in_specs=(
            P("seq", "tp"),
            P("seq", "tp"),
            P("seq", None),
            P("seq", None),
            P("seq", "tp"),
            P("tp"),
            P("tp"),
            P(),
            P(),
            P("tp"),
            P(),
        ),
        out_specs=P("seq", "tp"),
        check_vma=False,
    )
```

```python
import functools

import jax
import jax.numpy as jnp
from jax import lax
from jax.experimental import pallas as pl
from jax.experimental.pallas import tpu as pltpu
from jax.sharding import PartitionSpec as P

MESH = pl.DeviceIdType.MESH
LANES = 128
TILE = 8
ROWS16 = 16
epsilon = 1e-05


def kernel(
    seq_n,
    tp_n,
    head_width,
    inputs,
    gate_input,
    b_source,
    c_source,
    step_source,
    bias_source,
    decay_source,
    weight_source,
    conv_bias_source,
    gain_source,
    doc_lengths,
    output,
    step_raw,
    step_bias,
    decay_rate,
    conv_weight,
    conv_bias,
    norm_gain,
    result,
    xs,
    gates,
    source,
    halo,
    padded,
    own,
    from_pair,
    totals,
    received,
    prefixes,
    leaving,
    arrived,
    masked,
    mixed,
    gate_decay,
    squares,
    local_sem,
    small_sem,
    out_sem,
    halo_send,
    halo_recv,
    state_send,
    state_recv,
    square_send,
    square_recv,
):
    tokens = inputs.shape[0]
    chunks = xs.shape[0]
    half = chunks // 2
    state_width = b_source.shape[1]
    taps = weight_source.shape[0]
    bits = seq_n.bit_length() - 1
    me = lax.axis_index("seq")
    mine = lax.axis_index("tp")
    odd = lax.rem(me, 2)
    rows = state_width

    after = lax.rem(me + 1, seq_n)
    before = lax.rem(me + seq_n - 1, seq_n)
    partners = []
    for bit in range(bits):
        stride = 1 << bit
        partners.append(me + (1 - 2 * lax.rem(me // stride, 2)) * stride)
    barrier = pltpu.get_barrier_semaphore()
    for device in [after, before] + partners:
        pl.semaphore_signal(barrier, inc=1, device_id={"seq": device}, device_id_type=MESH)
    for ahead in range(1, tp_n):
        pl.semaphore_signal(
            barrier,
            inc=1,
            device_id={"tp": lax.rem(mine + ahead, tp_n)},
            device_id_type=MESH,
        )
    copies = [
        pltpu.make_async_copy(b_source, source.at[0], local_sem.at[0]),
        pltpu.make_async_copy(c_source, source.at[1], local_sem.at[1]),
    ]
    for copy in copies:
        copy.start()
    small = []
    for k, (src, dst) in enumerate(
        [
            (step_source, step_raw),
            (bias_source, step_bias),
            (decay_source, decay_rate),
            (weight_source, conv_weight),
            (conv_bias_source, conv_bias),
            (gain_source, norm_gain),
        ]
    ):
        small.append(pltpu.make_async_copy(src, dst, small_sem.at[k]))
        small[-1].start()
    x_copies, gate_copies = [], []
    for j in range(chunks):
        lanes = pl.ds(j * LANES, LANES)
        x_copies.append(
            pltpu.make_async_copy(inputs.at[:, lanes], xs.at[j], local_sem.at[2 + j])
        )
        x_copies[-1].start()
    for j in range(chunks):
        lanes = pl.ds(j * LANES, LANES)
        gate_copies.append(
            pltpu.make_async_copy(
                gate_input.at[:, lanes], gates.at[j], local_sem.at[2 + chunks + j]
            )
        )
        gate_copies[-1].start()

    first = me * tokens
    starts = []
    running = jnp.int32(0)
    for i in range(doc_lengths.shape[0]):
        starts.append(running)
        running = running + doc_lengths[i]

    def locate(position):
        chosen = jnp.zeros_like(position)
        for start in starts:
            chosen = jnp.maximum(chosen, jnp.where(position >= start, start, 0))
        return chosen

    position = first + lax.broadcasted_iota(jnp.int32, (tokens, LANES), 0)
    doc_start = locate(position)
    row_start = locate(first + lax.broadcasted_iota(jnp.int32, (TILE, tokens), 1))[:1]
    end_start = doc_start[tokens - 1 :, :1]

    for copy in small:
        copy.wait()
    step_size = jax.nn.softplus(jnp.transpose(step_raw[...]) + step_bias[...])
    log_decay = -step_size * decay_rate[...]
    row_ids = lax.broadcasted_iota(jnp.int32, (tokens, tokens), 0)
    column_ids = lax.broadcasted_iota(jnp.int32, (tokens, tokens), 1)
    causal = column_ids <= row_ids
    cumulated = jnp.dot(
        causal.astype(jnp.float32),
        log_decay,
        precision=lax.Precision.HIGHEST,
        preferred_element_type=jnp.float32,
    )
    heads = step_raw.shape[0]
    last = cumulated[tokens - 1 :]
    weighting = jnp.where(
        doc_start[:, :heads] == end_start, jnp.exp(last - cumulated) * step_size, 0.0
    )
    grow = jnp.exp(cumulated)
    out_decay = jnp.where(doc_start[:, :heads] < first, grow, 0.0)
    factor = jnp.where(end_start < first, jnp.exp(last), 0.0)
    shrink = jnp.transpose(jnp.exp(-cumulated) * step_size)
    low_half = lax.broadcasted_iota(jnp.int32, (1, LANES), 1) < head_width
    low_mask = low_half.astype(jnp.float32).astype(jnp.bfloat16)
    high_mask = (1.0 - low_half.astype(jnp.float32)).astype(jnp.bfloat16)

    def spread(values, j):
        return jnp.where(low_half, values[:, 2 * j : 2 * j + 1], values[:, 2 * j + 1 : 2 * j + 2])

    pl.semaphore_wait(barrier, 2 + bits + tp_n - 1)

    for copy in copies:
        copy.wait()
    halos = []
    for k in range(2):
        halos.append(
            pltpu.make_async_remote_copy(
                src_ref=source.at[k, pl.ds(tokens - ROWS16, ROWS16)],
                dst_ref=halo.at[k],
                send_sem=halo_send.at[k],
                recv_sem=halo_recv.at[k],
                device_id={"seq": after},
                device_id_type=MESH,
            )
        )
        halos[-1].start()

    for copy in halos:
        copy.wait()
    convolved = []
    for k in range(2):
        lanes = slice(k * state_width, (k + 1) * state_width)
        padded[k, 0:ROWS16, :] = halo[k].astype(jnp.float32)
        padded[k, ROWS16 : ROWS16 + tokens, :] = source[k].astype(jnp.float32)
        summed = jnp.broadcast_to(conv_bias[:, lanes], (tokens, state_width))
        for offset in range(taps):
            backward = taps - 1 - offset
            begin = ROWS16 - backward
            term = conv_weight[offset : offset + 1, lanes] * padded[k, begin : begin + tokens, :]
            summed = summed + jnp.where(position - backward >= doc_start, term, 0.0)
        convolved.append(jax.nn.silu(summed))
    b_conv = convolved[0].astype(jnp.bfloat16)
    c_conv = convolved[1].astype(jnp.bfloat16)
    b_across = jnp.transpose(convolved[0]).astype(jnp.bfloat16)

    def send(src, dst, stage, i, partner):
        return pltpu.make_async_remote_copy(
            src_ref=src,
            dst_ref=dst,
            send_sem=state_send.at[stage, i],
            recv_sem=state_recv.at[stage, i],
            device_id={"seq": partner},
            device_id_type=MESH,
        )

    def pending(stage):
        return [
            send(totals.at[stage - 1, i], received.at[stage - 1, i], stage, i, partners[stage])
            for i in range(half)
        ]

    stages = {stage: pending(stage) for stage in range(1, bits)}

    def end_state(j):
        x_copies[j].wait()
        weighted = (xs[j].astype(jnp.float32) * spread(weighting, j)).astype(jnp.bfloat16)
        own[j, :rows] = jnp.dot(b_across, weighted, preferred_element_type=jnp.float32)
        own[j, rows:] = jnp.broadcast_to(spread(factor, j), (TILE, LANES))

    def join(i):
        pair[i].wait()
        m = own[odd * half + i]
        p = from_pair[i]
        even = jnp.where(odd == 0, m, p)
        later = jnp.where(odd == 0, p, m)
        totals[0, i, :rows] = later[rows : rows + 1] * even[:rows] + later[:rows]
        totals[0, i, rows:] = later[rows:] * even[rows:]
        stages[1][i].start()

    pair = []
    for i in range(half):
        end_state(i)
        end_state(half + i)
        pair.append(send(own.at[(1 - odd) * half + i], from_pair.at[i], 0, i, partners[0]))
        pair[i].start()
        if i >= 2:
            join(i - 2)
    for i in range(max(half - 2, 0), half):
        join(i)

    products = lax.dot_general(
        c_conv, b_conv, (((1,), (1,)), ((), ())), preferred_element_type=jnp.float32
    )
    masked[...] = jnp.where(causal & (doc_start[:, :1] == row_start), products, 0.0)

    def diagonal(j):
        total = None
        x = xs[j]
        for k, mask in enumerate((low_mask, high_mask)):
            h = 2 * j + k
            scores = masked[...] * grow[:, h : h + 1] * shrink[h : h + 1, :]
            part = jnp.dot(
                scores.astype(jnp.bfloat16), x * mask, preferred_element_type=jnp.float32
            )
            total = part if total is None else total + part
        gate_copies[j].wait()
        gate = jax.nn.silu(gates[j].astype(jnp.float32))
        mixed[j] = total * gate
        gate_decay[j] = gate * spread(out_decay, j)

    def finish(j, state):
        from_state = jnp.dot(c_conv, state, preferred_element_type=jnp.float32)
        gated = mixed[j] + from_state * gate_decay[j]
        mixed[j] = gated
        return gated * gated

    done = 0
    last_stage = bits - 1
    square = jnp.zeros((tokens, LANES), jnp.float32)
    final = [send(leaving.at[i], arrived.at[i], bits, i, partners[0]) for i in range(half)]
    for stage in range(1, bits):
        bit = lax.rem(me // (1 << stage), 2)
        for i in range(half):
            while done < min(chunks, 2 * (i + 1)):
                diagonal(done)
                done += 1
            stages[stage][i].wait()
            p_state, p_factor = received[stage - 1, i, :rows], received[stage - 1, i, rows:]
            if stage < last_stage:
                m_state, m_factor = totals[stage - 1, i, :rows], totals[stage - 1, i, rows:]
                totals[stage, i, :rows] = jnp.where(
                    bit == 1, m_factor[:1] * p_state + m_state, p_factor[:1] * m_state + p_state
                )
                totals[stage, i, rows:] = m_factor * p_factor
                stages[stage + 1][i].start()
            if stage == 1:
                prefix = jnp.where(bit == 1, p_state, 0.0)
                prefix_factor = jnp.where(bit == 1, p_factor, 1.0)
            else:
                prefix, prefix_factor = prefixes[i, :rows], prefixes[i, rows:]
                prefix = jnp.where(bit == 1, prefix_factor[:1] * p_state + prefix, prefix)
                prefix_factor = jnp.where(bit == 1, prefix_factor * p_factor, prefix_factor)
            if stage < last_stage:
                prefixes[i, :rows] = prefix
                prefixes[i, rows:] = prefix_factor
                continue
            mine_here = own[odd * half + i]
            theirs = from_pair[i]
            even = jnp.where(odd == 0, mine_here, theirs)
            follows = even[rows : rows + 1] * prefix + even[:rows]
            leaving[i] = jnp.where(odd == 0, follows, prefix).astype(jnp.bfloat16)
            final[i].start()
            kept = jnp.where(odd == 0, prefix, follows).astype(jnp.bfloat16)
            square = square + finish(odd * half + i, kept)
    for i in range(half):
        final[i].wait()
        square = square + finish((1 - odd) * half + i, arrived[i])

    across = jnp.sum(jnp.transpose(square), axis=0, keepdims=True)
    squares[0] = jnp.broadcast_to(across, (TILE, tokens))
    sums = []
    for ahead in range(1, tp_n):
        sums.append(
            pltpu.make_async_remote_copy(
                src_ref=squares.at[0],
                dst_ref=squares.at[ahead],
                send_sem=square_send.at[ahead - 1],
                recv_sem=square_recv.at[ahead - 1],
                device_id={"tp": lax.rem(mine + ahead, tp_n)},
                device_id_type=MESH,
            )
        )
        sums[-1].start()
    for copy in sums:
        copy.wait()
    total = squares[0]
    for ahead in range(1, tp_n):
        total = total + squares[ahead]
    mean_square = total / (chunks * LANES * tp_n)
    scale = jnp.transpose(lax.rsqrt(mean_square + epsilon))[:, :1]
    scale = jnp.broadcast_to(scale, (tokens, LANES))
    leaves = []
    for j in range(chunks):
        lanes = pl.ds(j * LANES, LANES)
        gain = norm_gain[lanes].reshape(1, LANES)
        result[j] = (mixed[j] * scale * gain).astype(jnp.bfloat16)
        leaves.append(pltpu.make_async_copy(result.at[j], output.at[:, lanes], out_sem.at[j]))
        leaves[j].start()
    for copy in leaves:
        copy.wait()


def per_device(
    inputs,
    gate_input,
    b_source,
    c_source,
    step_raw,
    step_bias,
    decay_rate,
    conv_weight,
    conv_bias,
    norm_gain,
    doc_lengths,
):
    tokens, width = inputs.shape
    head_count = step_raw.shape[1]
    head_width = width // head_count
    state_width = b_source.shape[1]
    chunks = width // LANES
    half = chunks // 2
    seq_n, tp_n = lax.axis_size("seq"), lax.axis_size("tp")
    bits = seq_n.bit_length() - 1
    message = state_width + TILE
    whole = pl.BlockSpec(memory_space=pl.ANY)
    f32, bf16 = jnp.float32, jnp.bfloat16
    return pl.pallas_call(
        functools.partial(kernel, seq_n, tp_n, head_width),
        out_shape=jax.ShapeDtypeStruct((tokens, width), bf16),
        in_specs=[whole] * 10 + [pl.BlockSpec(memory_space=pltpu.SMEM)],
        out_specs=pl.BlockSpec(memory_space=pl.ANY),
        scratch_shapes=[
            pltpu.VMEM((head_count, tokens), f32),
            pltpu.VMEM((1, head_count), f32),
            pltpu.VMEM((1, head_count), f32),
            pltpu.VMEM(conv_weight.shape, f32),
            pltpu.VMEM((1, conv_bias.shape[0]), f32),
            pltpu.VMEM(norm_gain.shape, f32),
            pltpu.VMEM((chunks, tokens, LANES), bf16),
            pltpu.VMEM((chunks, tokens, LANES), bf16),
            pltpu.VMEM((chunks, tokens, LANES), bf16),
            pltpu.VMEM((2, tokens, state_width), bf16),
            pltpu.VMEM((2, ROWS16, state_width), bf16),
            pltpu.VMEM((2, tokens + ROWS16, state_width), f32),
            pltpu.VMEM((chunks, message, LANES), f32),
            pltpu.VMEM((half, message, LANES), f32),
            pltpu.VMEM((bits - 1, half, message, LANES), f32),
            pltpu.VMEM((bits - 1, half, message, LANES), f32),
            pltpu.VMEM((half, message, LANES), f32),
            pltpu.VMEM((half, state_width, LANES), bf16),
            pltpu.VMEM((half, state_width, LANES), bf16),
            pltpu.VMEM((tokens, tokens), f32),
            pltpu.VMEM((chunks, tokens, LANES), f32),
            pltpu.VMEM((chunks, tokens, LANES), f32),
            pltpu.VMEM((tp_n, TILE, tokens), f32),
            pltpu.SemaphoreType.DMA((2 + 2 * chunks,)),
            pltpu.SemaphoreType.DMA((6,)),
            pltpu.SemaphoreType.DMA((chunks,)),
            pltpu.SemaphoreType.DMA((2,)),
            pltpu.SemaphoreType.DMA((2,)),
            pltpu.SemaphoreType.DMA((bits + 1, half)),
            pltpu.SemaphoreType.DMA((bits + 1, half)),
            pltpu.SemaphoreType.DMA((tp_n - 1,)),
            pltpu.SemaphoreType.DMA((tp_n - 1,)),
        ],
        compiler_params=pltpu.CompilerParams(
            collective_id=0, has_side_effects=True, vmem_limit_bytes=60000 * 1024
        ),
    )(
        inputs,
        gate_input,
        b_source,
        c_source,
        step_raw.T,
        step_bias[None, :],
        decay_rate[None, :],
        conv_weight,
        conv_bias[None, :],
        norm_gain,
        doc_lengths,
    )


def solution(mesh):
    return jax.shard_map(
        per_device,
        mesh=mesh,
        in_specs=(
            P("seq", "tp"),
            P("seq", "tp"),
            P("seq", None),
            P("seq", None),
            P("seq", "tp"),
            P("tp"),
            P("tp"),
            P(),
            P(),
            P("tp"),
            P(),
        ),
        out_specs=P("seq", "tp"),
        check_vma=False,
    )
```
